32 devices in a mesh: tables: 8 (over z, y), cells: 4 (over x, core).
Axes of the slice: x: 2, y: 2, z: 4, core: 2. Of those that a mesh axis runs over, the one named last changes fastest.
Arguments:
- cells_in: bfloat16 [8, 128, 112, 192], P('tables', 'cells'), may hold values from -6 to 6
- train_count: int32 [8], P('tables'), may hold values from 32 to 96
- feat_count: int32 [8], P('tables'), may hold values from 28 to 112
- feat_qkv: bfloat16 [192, 576], replicated, may hold values from -2 to 2
- feat_proj: bfloat16 [192, 192], replicated, may hold values from -2 to 2
- row_qkv: bfloat16 [192, 576], replicated, may hold values from -2 to 2
- row_proj: bfloat16 [192, 192], replicated, may hold values from -0.4375 to 0.4375
- w_in: bfloat16 [192, 768], replicated, may hold values from -0.4375 to 0.4375
- w_out: bfloat16 [768, 192], replicated, may hold values from -0.21875 to 0.21875
- cotangent: bfloat16 [8, 128, 112, 192], P('tables', 'cells'), may hold values from -6 to 6
Outputs:
- cells_out: bfloat16 [8, 128, 112, 192], P('tables', 'cells')
- grad_in: float32 [192, 768], P(None, ('tables', 'cells'))
- grad_out: float32 [768, 192], P(('tables', 'cells'))
The draws below stay inside these ranges and needn't reach their ends.
All inputs are finite; a program needn't handle non-finite values.
Results may differ from the reference program's by a relative error of at most 0.018.
Values may be sent and summed in bfloat16 or wider, within the bound.
A program may use at most 128 MiB of HBM per device.

```python
import math
import jax
import jax.numpy as jnp
from jax import lax

E = 192
HEADS = 6
HEAD_DIM = 32
HID = 768
FEATS = 112
ROWS = 128
TABLES = 8


def base_weight(key, salt, rows, cols):
    values = jax.random.truncated_normal(jax.random.fold_in(key, salt), -6.0, 6.0, (rows, cols), jnp.float32)
    return values / jnp.float32(math.sqrt(rows))


def draw_feat_qkv(key, part):
    weight = base_weight(key, 31, E, 3 * E)
    return jnp.clip(weight, -2.0, 2.0).astype(jnp.bfloat16)


def draw_row_qkv(key, part):
    weight = base_weight(key, 41, E, 3 * E)
    return jnp.clip(weight, -2.0, 2.0).astype(jnp.bfloat16)


def draw_feat_proj(key, part):
    weight = base_weight(key, 51, E, E)
    return jnp.clip(weight, -2.0, 2.0).astype(jnp.bfloat16)


def draw_cells_in(key, part):
    cells = jax.random.truncated_normal(jax.random.fold_in(key, 21), -6.0, 6.0, (TABLES, ROWS, FEATS, E), jnp.float32)
    return jnp.clip(cells, -6.0, 6.0).astype(jnp.bfloat16)


def touch_ends(result, own_key, smallest, top_value):
    longest = result.shape.index(max(result.shape))
    spots = []
    for shift in (0, 1):
        where = [jax.random.randint(jax.random.fold_in(own_key, axis), (), 0, length) for axis, length in enumerate(result.shape)]
        where[longest] = (where[longest] + shift) % result.shape[longest]
        spots.append(tuple(where))
    return result.at[spots[0]].set(smallest).at[spots[1]].set(top_value)


def steps_of(own_key, shape, cuts, least, largest):
    loudness = 1.0
    for axis_at, shards_of in cuts:
        draws = jax.random.uniform(jax.random.fold_in(jax.random.fold_in(own_key, 6), axis_at), (shards_of,), jnp.float32, least / len(cuts), largest / len(cuts))
        loudness = loudness * jnp.repeat(jnp.exp(draws), shape[axis_at] // shards_of).reshape((-1,) + (1,) * (len(shape) - 1 - axis_at))
    return loudness


def bell_draw(rng, shape, scale, most, shards=(), kind=jnp.bfloat16):
    level = steps_of(rng, shape, shards, -0.22, 0.18) if shards else 1.0
    array = jax.random.normal(rng, shape, jnp.float32) * scale * level
    return jnp.minimum(jnp.maximum(array, -most), most).astype(kind)


def setup_inputs(seed: int = 0) -> dict:
    streams_of = jax.random.split(jax.random.key(seed), 11)
    cells_in = draw_cells_in(jax.random.fold_in(streams_of[10], 71), 0)
    train_count = touch_ends(jax.random.randint(streams_of[1], (TABLES,), ROWS // 4, ROWS - ROWS // 4 + 1), jax.random.fold_in(streams_of[1], 1), ROWS // 4, (ROWS - ROWS // 4 + 1) - 1).astype(jnp.int32)
    feat_count = touch_ends(jax.random.randint(streams_of[2], (TABLES,), FEATS // 4, FEATS + 1), jax.random.fold_in(streams_of[2], 1), FEATS // 4, FEATS).astype(jnp.int32)
    feat_qkv = draw_feat_qkv(jax.random.fold_in(streams_of[10], 71), 0)
    feat_proj = draw_feat_proj(jax.random.fold_in(streams_of[10], 71), 0)
    row_qkv = draw_row_qkv(jax.random.fold_in(streams_of[10], 71), 0)
    row_proj = bell_draw(streams_of[6], (E, E), E ** -0.5, 0.4375)
    w_in = bell_draw(streams_of[7], (E, HID), E ** -0.5, 0.4375)
    w_out = bell_draw(streams_of[8], (HID, E), HID ** -0.5, 0.21875)
    cotangent = bell_draw(streams_of[9], (TABLES, ROWS, FEATS, E), 1.0, 6.0, ((0, 8), (1, 4)))
    return dict(cells_in=cells_in, train_count=train_count, feat_count=feat_count, feat_qkv=feat_qkv, feat_proj=feat_proj, row_qkv=row_qkv, row_proj=row_proj, w_in=w_in, w_out=w_out, cotangent=cotangent)


def layer_norm(values):
    mean = lax.optimization_barrier(jnp.mean(values, axis=-1, keepdims=True))
    centred = values - mean
    var = lax.optimization_barrier(jnp.mean(centred * centred, axis=-1, keepdims=True))
    return centred / jnp.sqrt(var + 1e-05)

def feature_layer(block, feat_limit, weight_qkv, weight_proj):
    rows, feats, width = block.shape
    packed = jnp.dot(block.reshape(rows * feats, width), weight_qkv, preferred_element_type=jnp.float32)
    packed = packed.astype(jnp.bfloat16).reshape(rows, feats, 3, HEADS, HEAD_DIM).astype(jnp.float32)
    query, keys, values = (packed[:, :, 0], packed[:, :, 1], packed[:, :, 2])
    score = jnp.einsum('rfhd,rghd->rhfg', query, keys) / jnp.sqrt(jnp.float32(HEAD_DIM))
    keep = jnp.arange(feats, dtype=jnp.int32) < feat_limit
    score = jnp.where(keep[None, None, None, :], score, jnp.float32(-1e+30))
    probs = jax.nn.softmax(score, axis=-1).astype(jnp.bfloat16).astype(jnp.float32)
    attended = jnp.einsum('rhfg,rghd->rfhd', probs, values).astype(jnp.bfloat16)
    mixed = jnp.dot(attended.reshape(rows * feats, width), weight_proj, preferred_element_type=jnp.float32)
    total = block.reshape(rows * feats, width).astype(jnp.float32) + mixed
    return layer_norm(total).astype(jnp.bfloat16).reshape(rows, feats, width)

def row_single(column, train_limit, weight_qkv, weight_proj):
    rows, width = column.shape
    packed = jnp.dot(column, weight_qkv, preferred_element_type=jnp.float32)
    packed = packed.astype(jnp.bfloat16).reshape(rows, 3, HEADS, HEAD_DIM).astype(jnp.float32)
    query, keys, values = (packed[:, 0], packed[:, 1], packed[:, 2])
    score = jnp.einsum('ihd,jhd->hij', query, keys) / jnp.sqrt(jnp.float32(HEAD_DIM))
    keep = jnp.arange(rows, dtype=jnp.int32) < train_limit
    score = jnp.where(keep[None, None, :], score, jnp.float32(-1e+30))
    probs = jax.nn.softmax(score, axis=-1).astype(jnp.bfloat16).astype(jnp.float32)
    attended = jnp.einsum('hij,jhd->ihd', probs, values).astype(jnp.bfloat16).reshape(rows, width)
    mixed = jnp.dot(attended, weight_proj, preferred_element_type=jnp.float32)
    return layer_norm(column.astype(jnp.float32) + mixed).astype(jnp.bfloat16)

def exact_gelu(values):
    return jax.nn.gelu(values, approximate=False)

def reference(cells_in, train_count, feat_count, feat_qkv, feat_proj, row_qkv, row_proj, w_in, w_out, cotangent):

    def one_table(operands):
        block, cot_block, train_limit, feat_limit = operands
        mid = feature_layer(block, feat_limit, feat_qkv, feat_proj)
        columns = jnp.moveaxis(mid, 1, 0)
        normed_cols = lax.map(lambda column: row_single(column, train_limit, row_qkv, row_proj), columns)
        normed = jnp.moveaxis(normed_cols, 0, 1).reshape(-1, E)
        pre = jnp.dot(normed, w_in, preferred_element_type=jnp.float32)
        act_f, backward = jax.vjp(exact_gelu, pre)
        act = act_f.astype(jnp.bfloat16)
        output = (normed.astype(jnp.float32) + jnp.dot(act, w_out, preferred_element_type=jnp.float32)).astype(jnp.bfloat16)
        cot_flat = cot_block.reshape(-1, E)
        dact = jnp.dot(cot_flat, w_out.T, preferred_element_type=jnp.float32)
        dpre = backward(dact)[0].astype(jnp.bfloat16)
        part_in = jnp.dot(normed.T, dpre, preferred_element_type=jnp.float32)
        part_out = jnp.dot(act.T, cot_flat, preferred_element_type=jnp.float32)
        return (output.reshape(block.shape), part_in, part_out)
    outputs, parts_in, parts_out = lax.map(one_table, (cells_in, cotangent, train_count, feat_count))
    factor = 1.0 / jnp.sqrt(jnp.float32(TABLES * ROWS * FEATS))
    return (outputs, lax.optimization_barrier(jnp.sum(parts_in, axis=0)) * factor, lax.optimization_barrier(jnp.sum(parts_out, axis=0)) * factor)
```

```python
import math

import jax
import jax.numpy as jnp
from jax import lax
from jax.experimental import pallas as pl
from jax.experimental.pallas import tpu as pltpu
from jax.sharding import PartitionSpec as P

HEADS = 6
HEAD_DIM = 32
NEG = -1e30
LOG2E = math.log2(math.e)
SCALE = LOG2E / math.sqrt(HEAD_DIM)
AXES = ("tables", "cells")
F32 = jnp.float32
BF16 = jnp.bfloat16


def dot(a, b, ca, cb):
    return lax.dot_general(a, b, (((ca,), (cb,)), ((), ())), preferred_element_type=F32)


def layer_norm(values):
    mean = jnp.mean(values, axis=-1, keepdims=True)
    centred = values - mean
    var = jnp.mean(centred * centred, axis=-1, keepdims=True)
    return centred * lax.rsqrt(var + 1e-05)


def attend(x, w_t, w_proj, limit):
    n, width = x.shape
    packed = dot(w_t, x, 1, 1).astype(BF16)
    keep = lax.broadcasted_iota(jnp.int32, (n, 1), 0) < limit
    step = n if n <= 128 else 128
    heads = []
    for h in range(HEADS):
        lo = h * HEAD_DIM
        keys = packed[width + lo : width + lo + HEAD_DIM]
        vals = packed[2 * width + lo : 2 * width + lo + HEAD_DIM]
        cols = []
        for q0 in range(0, n, step):
            query = packed[lo : lo + HEAD_DIM, q0 : q0 + step]
            score = jnp.where(keep, dot(keys, query, 0, 0), NEG)
            top = jnp.max(score, axis=0, keepdims=True)
            prob = jnp.exp2((score - top) * SCALE)
            total = jnp.sum(prob, axis=0, keepdims=True)
            out = dot(vals, prob.astype(BF16), 1, 0)
            cols.append((out / total).astype(BF16))
        heads.append(cols[0] if len(cols) == 1 else jnp.concatenate(cols, axis=1))
    attended = jnp.concatenate(heads, axis=0)
    return layer_norm(x.astype(F32) + dot(attended, w_proj, 0, 0))


def feature_kernel(limit_ref, x_ref, w_ref, p_ref, o_ref, lo_ref, hi_ref):
    rows, feats, width = x_ref.shape
    limit = limit_ref[0]

    def body(r, carry):
        y = attend(x_ref[r], w_ref[...], p_ref[...], limit)
        spot = pl.ds(r, feats, stride=rows)
        lo_ref[spot, :] = y[:, :128]
        hi_ref[spot, :] = jnp.concatenate([y[:, 128:], jnp.zeros((feats, 256 - width), F32)], axis=1)
        return carry

    lax.fori_loop(0, rows, body, 0)
    o_ref[:, :, :128] = lo_ref[...].reshape(feats, rows, 128).astype(BF16)
    o_ref[:, :, 128:] = hi_ref[...].reshape(feats, rows, 128)[:, :, : width - 128].astype(BF16)


def row_kernel(limit_ref, x_ref, w_ref, p_ref, o_ref):
    groups, block, rows, width = x_ref.shape
    limit = limit_ref[0]

    def body(f, carry):
        x = x_ref[:, f].reshape(groups * rows, width)
        y = attend(x, w_ref[...], p_ref[...], limit)
        o_ref[:, f] = y.astype(BF16).reshape(groups, rows, width)
        return carry

    lax.fori_loop(0, block, body, 0)


def gelu_pair(x):
    bell = jnp.exp2(x * x * (-0.5 * LOG2E))
    t = 1.0 / (1.0 + (0.3275911 * math.sqrt(0.5)) * jnp.abs(x))
    poly = 0.5 * 1.061405429 * t + (0.5 * -1.453152027)
    poly = poly * t + (0.5 * 1.421413741)
    poly = poly * t + (0.5 * -0.284496736)
    poly = poly * t + (0.5 * 0.254829592)
    tail = poly * t * bell
    cdf = jnp.where(x < 0, tail, 1.0 - tail)
    return x * cdf, cdf + x * bell * (1.0 / math.sqrt(2.0 * math.pi))


def dense_kernel(factor, x_ref, c_ref, wi_ref, wo_ref, o_ref, gi_ref, go_ref, lo_ref, hi_ref, ai_ref, ao_ref):
    feats, rows, width = x_ref.shape
    cells = feats * rows
    step = pl.program_id(0)

    @pl.when(step == 0)
    def _():
        ai_ref[...] = jnp.zeros_like(ai_ref)
        ao_ref[...] = jnp.zeros_like(ao_ref)

    lo_ref[...] = x_ref[:, :, :128].astype(F32).reshape(cells, 128)
    hi_ref[:, : width - 128] = x_ref[:, :, 128:].astype(F32).reshape(cells, width - 128)
    group = 8

    def body(i, carry):
        parts = []
        for k in range(group):
            spot = pl.ds(i * group + k, feats, stride=rows)
            parts.append(jnp.concatenate([lo_ref[spot, :], hi_ref[spot, :][:, : width - 128]], axis=1).astype(BF16))
        normed = jnp.concatenate(parts, axis=0)
        here = pl.ds(i * group, group)
        cot = c_ref[here].reshape(group * feats, width)
        pre = dot(normed, wi_ref[...], 1, 0)
        act, slope = gelu_pair(pre)
        act = act.astype(BF16)
        out = normed.astype(F32) + dot(act, wo_ref[...], 1, 0)
        o_ref[here] = out.astype(BF16).reshape(group, feats, width)
        dpre = (dot(cot, wo_ref[...], 1, 1) * slope).astype(BF16)
        ai_ref[...] += dot(normed, dpre, 0, 0)
        ao_ref[...] += dot(cot, act, 0, 0)
        return carry

    lax.fori_loop(0, rows // group, body, 0)

    @pl.when(step == pl.num_programs(0) - 1)
    def _():
        gi_ref[...] = (ai_ref[...] * factor).T.astype(BF16)
        go_ref[...] = (ao_ref[...] * factor).T.astype(BF16)


def whole_spec(array):
    return pl.BlockSpec(array.shape, lambda i: (0,) * array.ndim)


def divisor(n, most):
    return max(k for k in range(1, most + 1) if n % k == 0)


def run_feature(limit, block, w_t, w_proj):
    rows, feats, width = block.shape
    part = 16 if rows % 16 == 0 else rows
    return pl.pallas_call(
        feature_kernel,
        grid=(rows // part,),
        out_shape=jax.ShapeDtypeStruct((feats, rows, width), BF16),
        in_specs=[
            pl.BlockSpec(memory_space=pltpu.SMEM),
            pl.BlockSpec((part, feats, width), lambda i: (i, 0, 0)),
            whole_spec(w_t),
            whole_spec(w_proj),
        ],
        out_specs=pl.BlockSpec((feats, part, width), lambda i: (0, i, 0)),
        scratch_shapes=[pltpu.VMEM((feats * part, 128), F32)] * 2,
        cost_estimate=pl.CostEstimate(flops=4 * 10**9, bytes_accessed=4 * 10**6, transcendentals=0),
        name="feature",
    )(limit, block, w_t, w_proj)


def run_row(limit, columns, w_t, w_proj):
    groups, feats, rows, width = columns.shape
    part = divisor(feats, 4)
    spec = pl.BlockSpec((groups, part, rows, width), lambda i: (0, i, 0, 0))
    return pl.pallas_call(
        row_kernel,
        grid=(feats // part,),
        out_shape=jax.ShapeDtypeStruct(columns.shape, BF16),
        in_specs=[pl.BlockSpec(memory_space=pltpu.SMEM), spec, whole_spec(w_t), whole_spec(w_proj)],
        out_specs=spec,
        cost_estimate=pl.CostEstimate(flops=4 * 10**9, bytes_accessed=4 * 10**6, transcendentals=0),
        name="row",
    )(limit, columns, w_t, w_proj)


def run_dense(factor, normed, cot, w_in, w_out):
    feats, rows, width = normed.shape
    hidden = w_in.shape[1]
    part = 16 if feats % 16 == 0 else feats
    natural = pl.BlockSpec((rows, part, width), lambda i: (0, i, 0))
    grad = pl.BlockSpec((hidden, width), lambda i: (0, 0))
    return pl.pallas_call(
        lambda *refs: dense_kernel(factor, *refs),
        grid=(feats // part,),
        out_shape=[
            jax.ShapeDtypeStruct((rows, feats, width), BF16),
            jax.ShapeDtypeStruct((hidden, width), BF16),
            jax.ShapeDtypeStruct((hidden, width), BF16),
        ],
        in_specs=[
            pl.BlockSpec((part, rows, width), lambda i: (i, 0, 0)),
            natural,
            whole_spec(w_in),
            whole_spec(w_out),
        ],
        out_specs=[natural, grad, grad],
        scratch_shapes=[pltpu.VMEM((part * rows, 128), F32)] * 2 + [pltpu.VMEM((width, hidden), F32)] * 2,
        cost_estimate=pl.CostEstimate(flops=8 * 10**9, bytes_accessed=6 * 10**6, transcendentals=0),
        name="dense",
    )(normed, cot, w_in, w_out)


def per_device(
    cells_in, train_count, feat_count, feat_qkv, feat_proj, row_qkv, row_proj, w_in, w_out, cotangent
):
    block = cells_in[0]
    rows, feats, width = block.shape
    groups = lax.axis_size("cells")
    devices = groups * lax.axis_size("tables")
    mid = run_feature(feat_count, block, feat_qkv.T, feat_proj)
    columns = mid.reshape(groups, feats // groups, rows, width)
    columns = lax.all_to_all(columns, "cells", split_axis=0, concat_axis=0, tiled=True)
    done = run_row(train_count, columns, row_qkv.T, row_proj)
    normed = lax.all_to_all(done, "cells", split_axis=0, concat_axis=0, tiled=True)
    factor = 1.0 / math.sqrt(devices * rows * feats)
    output, part_in, part_out = run_dense(
        factor, normed.reshape(feats, rows, width), cotangent[0], w_in, w_out
    )
    own = part_in.shape[0] // devices
    sends = jnp.concatenate(
        [part_in.reshape(devices, own, width), part_out.reshape(devices, own, width)], axis=1
    )
    got = lax.all_to_all(sends, AXES, split_axis=0, concat_axis=0, tiled=True)
    total = jnp.sum(got.astype(F32), axis=0)
    return output[None], total[:own].T, total[own:]


def solution(mesh):
    return jax.shard_map(
        per_device,
        mesh=mesh,
        in_specs=(
            P("tables", "cells", None, None),
            P("tables"),
            P("tables"),
            P(),
            P(),
            P(),
            P(),
            P(),
            P(),
            P("tables", "cells", None, None),
        ),
        out_specs=(
            P("tables", "cells", None, None),
            P(None, ("tables", "cells")),
            P(("tables", "cells"), None),
        ),
        check_vma=False,
    )
```

```python
import math

import jax
import jax.numpy as jnp
from jax import lax
from jax.experimental import pallas as pl
from jax.experimental.pallas import tpu as pltpu
from jax.sharding import PartitionSpec as P

HEADS = 6
HEAD_DIM = 32
NEG = -1e30
UNROLL = 8
GROUP = 4
LOG2E = math.log2(math.e)
SCALE = LOG2E / math.sqrt(HEAD_DIM)
AXES = ("tables", "cells")
F32 = jnp.float32
BF16 = jnp.bfloat16


def dot(a, b, ca, cb):
    return lax.dot_general(a, b, (((ca,), (cb,)), ((), ())), preferred_element_type=F32)


def layer_norm(values, axis):
    mean = jnp.mean(values, axis=axis, keepdims=True)
    centred = values - mean
    var = jnp.mean(centred * centred, axis=axis, keepdims=True)
    return centred * lax.rsqrt(var + 1e-05)


def attend(packs, limit):
    width, n = packs[0].shape[0] // 3, packs[0].shape[1]
    keep = lax.broadcasted_iota(jnp.int32, (n, 1), 0) < limit
    step = n if n <= 128 else 128
    jobs = [(i, h, q0) for i in range(len(packs)) for h in range(HEADS) for q0 in range(0, n, step)]
    scores, probs, outs = [], [], []
    for i, h, q0 in jobs:
        lo = h * HEAD_DIM
        keys = packs[i][width + lo : width + lo + HEAD_DIM]
        query = packs[i][lo : lo + HEAD_DIM, q0 : q0 + step]
        scores.append(dot(keys, query, 0, 0))
    for score in scores:
        score = jnp.where(keep, score, NEG)
        prob = jnp.exp2((score - jnp.max(score, axis=0, keepdims=True)) * SCALE)
        probs.append((prob.astype(BF16), 1.0 / jnp.sum(prob, axis=0, keepdims=True)))
    for (i, h, q0), (prob, inverse) in zip(jobs, probs):
        lo = 2 * width + h * HEAD_DIM
        outs.append((dot(packs[i][lo : lo + HEAD_DIM], prob, 1, 0), inverse))
    outs = [(out * inverse).astype(BF16) for out, inverse in outs]
    blocks = n // step
    result = []
    for i in range(len(packs)):
        heads = []
        for h in range(HEADS):
            at = (i * HEADS + h) * blocks
            cols = outs[at : at + blocks]
            heads.append(cols[0] if blocks == 1 else jnp.concatenate(cols, axis=1))
        result.append(jnp.concatenate(heads, axis=0))
    return result


def feature_kernel(limit_ref, x_ref, wn_ref, pn_ref, o_ref, lo_ref, hi_ref, w_ref, p_ref):
    rows, width, feats = x_ref.shape
    limit = limit_ref[0]

    @pl.when(pl.program_id(0) == 0)
    def _():
        w_ref[...] = wn_ref[...].T
        p_ref[...] = pn_ref[...].T

    unroll = UNROLL if rows % UNROLL == 0 else 1

    def body(i, carry):
        spots = [i * unroll + k for k in range(unroll)]
        cells = [x_ref[r] for r in spots]
        packs = [dot(w_ref[...], x, 1, 0).astype(BF16) for x in cells]
        attended = attend(packs, limit)
        mixed = [dot(p_ref[...], a, 1, 0) for a in attended]
        for r, x, m in zip(spots, cells, mixed):
            y = layer_norm(x.astype(F32) + m, 0)
            spot = pl.ds(r, feats, stride=rows)
            lo_ref[spot, :] = y[:128].T
            hi_ref[spot, :] = jnp.concatenate([y[128:], jnp.zeros((256 - width, feats), F32)], axis=0).T
        return carry

    lax.fori_loop(0, rows // unroll, body, 0)
    o_ref[:, :, :128] = lo_ref[...].reshape(feats, rows, 128).astype(BF16)
    o_ref[:, :, 128:] = hi_ref[...].reshape(feats, rows, 128)[:, :, : width - 128].astype(BF16)


def row_kernel(limit_ref, x_ref, wn_ref, p_ref, o_ref, w_ref):
    groups, block, rows, width = x_ref.shape
    limit = limit_ref[0]

    @pl.when(pl.program_id(0) == 0)
    def _():
        w_ref[...] = wn_ref[...].T


    unroll = block

    def body(i, carry):
        spots = [i * unroll + k for k in range(unroll)]
        cells = [x_ref[:, f].reshape(groups * rows, width) for f in spots]
        packs = [dot(w_ref[...], x, 1, 1).astype(BF16) for x in cells]
        attended = attend(packs, limit)
        mixed = [dot(a, p_ref[...], 0, 0) for a in attended]
        for f, x, m in zip(spots, cells, mixed):
            y = layer_norm(x.astype(F32) + m, -1)
            o_ref[:, f] = y.astype(BF16).reshape(groups, rows, width)
        return carry

    lax.fori_loop(0, block // unroll, body, 0)


def gelu_pair(x):
    bell = jnp.exp2(x * x * (-0.5 * LOG2E))
    t = 1.0 / (1.0 + (0.3275911 * math.sqrt(0.5)) * jnp.abs(x))
    poly = 0.5 * 1.061405429 * t + (0.5 * -1.453152027)
    poly = poly * t + (0.5 * 1.421413741)
    poly = poly * t + (0.5 * -0.284496736)
    poly = poly * t + (0.5 * 0.254829592)
    tail = poly * t * bell
    cdf = jnp.where(x < 0, tail, 1.0 - tail)
    return x * cdf, cdf + x * bell * (1.0 / math.sqrt(2.0 * math.pi))


def dense_kernel(factor, x_ref, c_ref, wi_ref, wo_ref, o_ref, gi_ref, go_ref, lo_ref, hi_ref, ai_ref, ao_ref):
    feats, rows, width = x_ref.shape
    cells = feats * rows
    step = pl.program_id(0)

    @pl.when(step == 0)
    def _():
        ai_ref[...] = jnp.zeros_like(ai_ref)
        ao_ref[...] = jnp.zeros_like(ao_ref)

    lo_ref[...] = x_ref[:, :, :128].astype(F32).reshape(cells, 128)
    hi_ref[:, : width - 128] = x_ref[:, :, 128:].astype(F32).reshape(cells, width - 128)
    group = GROUP if rows % GROUP == 0 else 1

    def body(i, carry):
        spots = [i * group + k for k in range(group)]
        parts, cots = [], []
        for r in spots:
            spot = pl.ds(r, feats, stride=rows)
            parts.append(jnp.concatenate([lo_ref[spot, :], hi_ref[spot, :][:, : width - 128]], axis=1).astype(BF16))
            cots.append(c_ref[r].T)
        normed = jnp.concatenate(parts, axis=0)
        cot = jnp.concatenate(cots, axis=0)
        act, slope = gelu_pair(dot(normed, wi_ref[...], 1, 0))
        act = act.astype(BF16)
        dpre = (dot(cot, wo_ref[...], 1, 0) * slope).astype(BF16)
        out = normed.astype(F32) + dot(act, wo_ref[...], 1, 1)
        for k, r in enumerate(spots):
            o_ref[r] = out[k * feats : (k + 1) * feats].T.astype(BF16)
        ai_ref[...] += dot(normed, dpre, 0, 0)
        ao_ref[...] += dot(cot, act, 0, 0)
        return carry

    lax.fori_loop(0, rows // group, body, 0)

    @pl.when(step == pl.num_programs(0) - 1)
    def _():
        gi_ref[...] = (ai_ref[...] * factor).T.astype(BF16)
        go_ref[...] = (ao_ref[...] * factor).T.astype(BF16)


def whole_spec(array):
    return pl.BlockSpec(array.shape, lambda i: (0,) * array.ndim)


def divisor(n, most):
    return max(k for k in range(1, most + 1) if n % k == 0)


def run_feature(limit, block, w_qkv, w_proj):
    rows, width, feats = block.shape
    part = 16 if rows % 16 == 0 else rows
    return pl.pallas_call(
        feature_kernel,
        grid=(rows // part,),
        out_shape=jax.ShapeDtypeStruct((feats, rows, width), BF16),
        in_specs=[
            pl.BlockSpec(memory_space=pltpu.SMEM),
            pl.BlockSpec((part, width, feats), lambda i: (i, 0, 0)),
            whole_spec(w_qkv),
            whole_spec(w_proj),
        ],
        out_specs=pl.BlockSpec((feats, part, width), lambda i: (0, i, 0)),
        scratch_shapes=[pltpu.VMEM((feats * part, 128), F32)] * 2
        + [pltpu.VMEM(w_qkv.shape[::-1], BF16), pltpu.VMEM(w_proj.shape[::-1], BF16)],
        cost_estimate=pl.CostEstimate(flops=4 * 10**9, bytes_accessed=4 * 10**6, transcendentals=0),
        name="feature",
    )(limit, block, w_qkv, w_proj)


def run_row(limit, columns, w_qkv, w_proj):
    groups, feats, rows, width = columns.shape
    part = divisor(feats, 7 if groups * rows <= 128 else 1)
    spec = pl.BlockSpec((groups, part, rows, width), lambda i: (0, i, 0, 0))
    return pl.pallas_call(
        row_kernel,
        grid=(feats // part,),
        out_shape=jax.ShapeDtypeStruct(columns.shape, BF16),
        in_specs=[pl.BlockSpec(memory_space=pltpu.SMEM), spec, whole_spec(w_qkv), whole_spec(w_proj)],
        out_specs=spec,
        scratch_shapes=[pltpu.VMEM(w_qkv.shape[::-1], BF16)],
        cost_estimate=pl.CostEstimate(flops=4 * 10**9, bytes_accessed=4 * 10**6, transcendentals=0),
        name="row",
    )(limit, columns, w_qkv, w_proj)


def run_dense(factor, normed, cot, w_in, w_out):
    feats, rows, width = normed.shape
    hidden = w_in.shape[1]
    part = 8 if rows % 8 == 0 else rows
    natural = pl.BlockSpec((part, width, feats), lambda i: (i, 0, 0))
    grad = pl.BlockSpec((hidden, width), lambda i: (0, 0))
    return pl.pallas_call(
        lambda *refs: dense_kernel(factor, *refs),
        grid=(rows // part,),
        out_shape=[
            jax.ShapeDtypeStruct((rows, width, feats), BF16),
            jax.ShapeDtypeStruct((hidden, width), BF16),
            jax.ShapeDtypeStruct((hidden, width), BF16),
        ],
        in_specs=[
            pl.BlockSpec((feats, part, width), lambda i: (0, i, 0)),
            natural,
            whole_spec(w_in),
            whole_spec(w_out),
        ],
        out_specs=[natural, grad, grad],
        scratch_shapes=[pltpu.VMEM((part * feats, 128), F32)] * 2 + [pltpu.VMEM((width, hidden), F32)] * 2,
        cost_estimate=pl.CostEstimate(flops=8 * 10**9, bytes_accessed=6 * 10**6, transcendentals=0),
        name="dense",
    )(normed, cot, w_in, w_out)


def per_device(
    cells_in, train_count, feat_count, feat_qkv, feat_proj, row_qkv, row_proj, w_in, w_out, cotangent
):
    block = cells_in[0]
    rows, feats, width = block.shape
    groups = lax.axis_size("cells")
    devices = groups * lax.axis_size("tables")
    mid = run_feature(feat_count, jnp.swapaxes(block, 1, 2), feat_qkv, feat_proj)
    columns = mid.reshape(groups, feats // groups, rows, width)
    columns = lax.all_to_all(columns, "cells", split_axis=0, concat_axis=0, tiled=True)
    done = run_row(train_count, columns, row_qkv, row_proj)
    normed = lax.all_to_all(done, "cells", split_axis=0, concat_axis=0, tiled=True)
    factor = 1.0 / math.sqrt(devices * rows * feats)
    output, part_in, part_out = run_dense(
        factor, normed.reshape(feats, rows, width), jnp.swapaxes(cotangent[0], 1, 2), w_in, w_out.T
    )
    own = part_in.shape[0] // devices
    sends = jnp.concatenate(
        [part_in.reshape(devices, own, width), part_out.reshape(devices, own, width)], axis=1
    )
    got = lax.all_to_all(sends, AXES, split_axis=0, concat_axis=0, tiled=True)
    total = jnp.sum(got.astype(F32), axis=0)
    return jnp.swapaxes(output, 1, 2)[None], total[:own].T, total[own:]


def solution(mesh):
    return jax.shard_map(
        per_device,
        mesh=mesh,
        in_specs=(
            P("tables", "cells", None, None),
            P("tables"),
            P("tables"),
            P(),
            P(),
            P(),
            P(),
            P(),
            P(),
            P("tables", "cells", None, None),
        ),
        out_specs=(
            P("tables", "cells", None, None),
            P(None, ("tables", "cells")),
            P(("tables", "cells"), None),
        ),
        check_vma=False,
    )
```

```python
import math

import jax
import jax.numpy as jnp
from jax import lax
from jax.experimental import pallas as pl
from jax.experimental.pallas import tpu as pltpu
from jax.sharding import PartitionSpec as P

HEADS = 6
HEAD_DIM = 32
NEG = -1e30
UNROLL = 8
GROUP = 4
LOG2E = math.log2(math.e)
SCALE = LOG2E / math.sqrt(HEAD_DIM)
AXES = ("tables", "cells")
F32 = jnp.float32
BF16 = jnp.bfloat16


def dot(a, b, ca, cb):
    return lax.dot_general(a, b, (((ca,), (cb,)), ((), ())), preferred_element_type=F32)


def layer_norm(values, axis):
    mean = jnp.mean(values, axis=axis, keepdims=True)
    centred = values - mean
    var = jnp.mean(centred * centred, axis=axis, keepdims=True)
    return centred * lax.rsqrt(var + 1e-05)


def attend(packs, limit):
    width, n = packs[0].shape[0] // 3, packs[0].shape[1]
    keep = lax.broadcasted_iota(jnp.int32, (n, 1), 0) < limit
    step = n if n <= 128 else 128
    jobs = [(i, h, q0) for i in range(len(packs)) for h in range(HEADS) for q0 in range(0, n, step)]
    scores, probs, outs = [], [], []
    for i, h, q0 in jobs:
        lo = h * HEAD_DIM
        keys = packs[i][width + lo : width + lo + HEAD_DIM]
        query = packs[i][lo : lo + HEAD_DIM, q0 : q0 + step]
        scores.append(dot(keys, query, 0, 0))
    for score in scores:
        score = jnp.where(keep, score, NEG)
        prob = jnp.exp2((score - jnp.max(score, axis=0, keepdims=True)) * SCALE)
        probs.append((prob.astype(BF16), 1.0 / jnp.sum(prob, axis=0, keepdims=True)))
    for (i, h, q0), (prob, inverse) in zip(jobs, probs):
        lo = 2 * width + h * HEAD_DIM
        outs.append((dot(packs[i][lo : lo + HEAD_DIM], prob, 1, 0), inverse))
    outs = [(out * inverse).astype(BF16) for out, inverse in outs]
    blocks = n // step
    result = []
    for i in range(len(packs)):
        heads = []
        for h in range(HEADS):
            at = (i * HEADS + h) * blocks
            cols = outs[at : at + blocks]
            heads.append(cols[0] if blocks == 1 else jnp.concatenate(cols, axis=1))
        result.append(jnp.concatenate(heads, axis=0))
    return result


def feature_kernel(limit_ref, x_ref, wn_ref, pn_ref, o_ref, lo_ref, hi_ref, w_ref, p_ref):
    rows, width, feats = x_ref.shape
    limit = limit_ref[0]

    @pl.when(pl.program_id(0) == 0)
    def _():
        w_ref[...] = wn_ref[...].T
        p_ref[...] = pn_ref[...].T

    unroll = UNROLL if rows % UNROLL == 0 else 1

    def body(i, carry):
        spots = [i * unroll + k for k in range(unroll)]
        cells = [x_ref[r] for r in spots]
        packs = [dot(w_ref[...], x, 1, 0).astype(BF16) for x in cells]
        attended = attend(packs, limit)
        mixed = [dot(p_ref[...], a, 1, 0) for a in attended]
        for r, x, m in zip(spots, cells, mixed):
            y = layer_norm(x.astype(F32) + m, 0)
            spot = pl.ds(r, feats, stride=rows)
            lo_ref[spot, :] = y[:128].T
            hi_ref[spot, :] = jnp.concatenate([y[128:], jnp.zeros((256 - width, feats), F32)], axis=0).T
        return carry

    lax.fori_loop(0, rows // unroll, body, 0)
    o_ref[:, :, :128] = lo_ref[...].reshape(feats, rows, 128).astype(BF16)
    o_ref[:, :, 128:] = hi_ref[...].reshape(feats, rows, 128)[:, :, : width - 128].astype(BF16)


def row_kernel(limit_ref, x_ref, wn_ref, p_ref, o_ref, w_ref):
    groups, block, rows, width = x_ref.shape
    limit = limit_ref[0]

    @pl.when(pl.program_id(0) == 0)
    def _():
        w_ref[...] = wn_ref[...].T


    unroll = block

    def body(i, carry):
        spots = [i * unroll + k for k in range(unroll)]
        cells = [x_ref[:, f].reshape(groups * rows, width) for f in spots]
        packs = [dot(w_ref[...], x, 1, 1).astype(BF16) for x in cells]
        attended = attend(packs, limit)
        mixed = [dot(a, p_ref[...], 0, 0) for a in attended]
        for f, x, m in zip(spots, cells, mixed):
            y = layer_norm(x.astype(F32) + m, -1)
            o_ref[:, f] = y.astype(BF16).reshape(groups, rows, width)
        return carry

    lax.fori_loop(0, block // unroll, body, 0)


def gelu_pair(x):
    bell = jnp.exp2(x * x * (-0.5 * LOG2E))
    t = 1.0 / (1.0 + (0.3275911 * math.sqrt(0.5)) * jnp.abs(x))
    poly = 0.5 * 1.061405429 * t + (0.5 * -1.453152027)
    poly = poly * t + (0.5 * 1.421413741)
    poly = poly * t + (0.5 * -0.284496736)
    poly = poly * t + (0.5 * 0.254829592)
    tail = poly * t * bell
    cdf = jnp.where(x < 0, tail, 1.0 - tail)
    return x * cdf, cdf + x * bell * (1.0 / math.sqrt(2.0 * math.pi))


def dense_kernel(factor, x_ref, c_ref, wi_ref, wo_ref, o_ref, gi_ref, go_ref, lo_ref, hi_ref, ai_ref, ao_ref):
    feats, rows, width = x_ref.shape
    cells = feats * rows
    step = pl.program_id(0)

    @pl.when(step == 0)
    def _():
        ai_ref[...] = jnp.zeros_like(ai_ref)
        ao_ref[...] = jnp.zeros_like(ao_ref)

    lo_ref[...] = x_ref[:, :, :128].astype(F32).reshape(cells, 128)
    hi_ref[:, : width - 128] = x_ref[:, :, 128:].astype(F32).reshape(cells, width - 128)
    group = GROUP if rows % GROUP == 0 else 1

    def body(i, carry):
        spots = [i * group + k for k in range(group)]
        parts, cots = [], []
        for r in spots:
            spot = pl.ds(r, feats, stride=rows)
            parts.append(jnp.concatenate([lo_ref[spot, :], hi_ref[spot, :][:, : width - 128]], axis=1).astype(BF16))
            cots.append(c_ref[r].T)
        normed = jnp.concatenate(parts, axis=0)
        cot = jnp.concatenate(cots, axis=0)
        act, slope = gelu_pair(dot(normed, wi_ref[...], 1, 0))
        act = act.astype(BF16)
        dpre = (dot(cot, wo_ref[...], 1, 0) * slope).astype(BF16)
        out = normed.astype(F32) + dot(act, wo_ref[...], 1, 1)
        for k, r in enumerate(spots):
            o_ref[r] = out[k * feats : (k + 1) * feats].T.astype(BF16)
        ai_ref[...] += dot(normed, dpre, 0, 0)
        ao_ref[...] += dot(cot, act, 0, 0)
        return carry

    lax.fori_loop(0, rows // group, body, 0)

    @pl.when(step == pl.num_programs(0) - 1)
    def _():
        gi_ref[...] = (ai_ref[...] * factor).T.astype(BF16)
        go_ref[...] = (ao_ref[...] * factor).T.astype(BF16)


def whole_spec(array):
    return pl.BlockSpec(array.shape, lambda i: (0,) * array.ndim)


def divisor(n, most):
    return max(k for k in range(1, most + 1) if n % k == 0)


def run_feature(limit, block, w_qkv, w_proj):
    rows, width, feats = block.shape
    part = 16 if rows % 16 == 0 else rows
    return pl.pallas_call(
        feature_kernel,
        grid=(rows // part,),
        out_shape=jax.ShapeDtypeStruct((feats, rows, width), BF16),
        in_specs=[
            pl.BlockSpec(memory_space=pltpu.SMEM),
            pl.BlockSpec((part, width, feats), lambda i: (i, 0, 0)),
            whole_spec(w_qkv),
            whole_spec(w_proj),
        ],
        out_specs=pl.BlockSpec((feats, part, width), lambda i: (0, i, 0)),
        scratch_shapes=[pltpu.VMEM((feats * part, 128), F32)] * 2
        + [pltpu.VMEM(w_qkv.shape[::-1], BF16), pltpu.VMEM(w_proj.shape[::-1], BF16)],
        cost_estimate=pl.CostEstimate(flops=4 * 10**9, bytes_accessed=4 * 10**6, transcendentals=0),
        name="feature",
    )(limit, block, w_qkv, w_proj)


def run_row(limit, columns, w_qkv, w_proj):
    groups, feats, rows, width = columns.shape
    part = divisor(feats, 7 if groups * rows <= 128 else 1)
    spec = pl.BlockSpec((groups, part, rows, width), lambda i: (0, i, 0, 0))
    return pl.pallas_call(
        row_kernel,
        grid=(feats // part,),
        out_shape=jax.ShapeDtypeStruct(columns.shape, BF16),
        in_specs=[pl.BlockSpec(memory_space=pltpu.SMEM), spec, whole_spec(w_qkv), whole_spec(w_proj)],
        out_specs=spec,
        scratch_shapes=[pltpu.VMEM(w_qkv.shape[::-1], BF16)],
        cost_estimate=pl.CostEstimate(flops=4 * 10**9, bytes_accessed=4 * 10**6, transcendentals=0),
        name="row",
    )(limit, columns, w_qkv, w_proj)


def run_dense(factor, normed, cot, w_in, w_out):
    feats, rows, width = normed.shape
    hidden = w_in.shape[1]
    part = 8 if rows % 8 == 0 else rows
    natural = pl.BlockSpec((part, width, feats), lambda i: (i, 0, 0))
    grad = pl.BlockSpec((hidden, width), lambda i: (0, 0))
    return pl.pallas_call(
        lambda *refs: dense_kernel(factor, *refs),
        grid=(rows // part,),
        out_shape=[
            jax.ShapeDtypeStruct((rows, width, feats), BF16),
            jax.ShapeDtypeStruct((hidden, width), BF16),
            jax.ShapeDtypeStruct((hidden, width), BF16),
        ],
        in_specs=[
            pl.BlockSpec((feats, part, width), lambda i: (0, i, 0)),
            natural,
            whole_spec(w_in),
            whole_spec(w_out),
        ],
        out_specs=[natural, grad, grad],
        scratch_shapes=[pltpu.VMEM((part * feats, 128), F32)] * 2 + [pltpu.VMEM((width, hidden), F32)] * 2,
        cost_estimate=pl.CostEstimate(flops=8 * 10**9, bytes_accessed=6 * 10**6, transcendentals=0),
        name="dense",
    )(normed, cot, w_in, w_out)


def exchange_kernel(axes, sizes, x_ref, o_ref, own_ref, own_sem, send_sem, recv_sem):
    count = math.prod(sizes)
    me = 0
    for axis, size in zip(axes, sizes):
        me = me * size + lax.axis_index(axis)

    def target(k):
        peer = lax.rem(me + k, count)
        if len(axes) == 1:
            return peer, {axes[0]: peer}
        return peer, {axes[0]: lax.div(peer, sizes[1]), axes[1]: lax.rem(peer, sizes[1])}

    def copy(k):
        peer, device = target(k)
        return pltpu.make_async_remote_copy(
            src_ref=x_ref.at[peer],
            dst_ref=o_ref.at[me],
            send_sem=send_sem.at[k],
            recv_sem=recv_sem.at[k],
            device_id=device,
            device_id_type=pl.DeviceIdType.MESH,
        )

    barrier = pltpu.get_barrier_semaphore()

    def greet(k, carry):
        pl.semaphore_signal(barrier, inc=1, device_id=target(k)[1], device_id_type=pl.DeviceIdType.MESH)
        return carry

    def start(k, carry):
        copy(k).start()
        return carry

    def finish(k, carry):
        copy(k).wait()
        return carry

    load = pltpu.make_async_copy(x_ref.at[me], own_ref, own_sem.at[0])
    load.start()
    lax.fori_loop(1, count, greet, 0)
    pl.semaphore_wait(barrier, count - 1)
    lax.fori_loop(1, count, start, 0)
    load.wait()
    store = pltpu.make_async_copy(own_ref, o_ref.at[me], own_sem.at[1])
    store.start()
    lax.fori_loop(1, count, finish, 0)
    store.wait()


def exchange(array, axes, ident):
    sizes = [lax.axis_size(axis) for axis in axes]
    return pl.pallas_call(
        lambda *refs: exchange_kernel(axes, sizes, *refs),
        out_shape=jax.ShapeDtypeStruct(array.shape, array.dtype),
        in_specs=[pl.BlockSpec(memory_space=pl.ANY)],
        out_specs=pl.BlockSpec(memory_space=pl.ANY),
        scratch_shapes=[
            pltpu.VMEM(array.shape[1:], array.dtype),
            pltpu.SemaphoreType.DMA((2,)),
            pltpu.SemaphoreType.DMA((array.shape[0],)),
            pltpu.SemaphoreType.DMA((array.shape[0],)),
        ],
        compiler_params=pltpu.CompilerParams(collective_id=ident, has_side_effects=True),
        name="exchange%d" % ident,
    )(array)


def per_device(
    cells_in, train_count, feat_count, feat_qkv, feat_proj, row_qkv, row_proj, w_in, w_out, cotangent
):
    block = cells_in[0]
    rows, feats, width = block.shape
    groups = lax.axis_size("cells")
    devices = groups * lax.axis_size("tables")
    mid = run_feature(feat_count, jnp.swapaxes(block, 1, 2), feat_qkv, feat_proj)
    columns = mid.reshape(groups, feats // groups, rows, width)
    columns = exchange(columns, ("cells",), 0)
    done = run_row(train_count, columns, row_qkv, row_proj)
    normed = exchange(done, ("cells",), 1)
    factor = 1.0 / math.sqrt(devices * rows * feats)
    output, part_in, part_out = run_dense(
        factor, normed.reshape(feats, rows, width), jnp.swapaxes(cotangent[0], 1, 2), w_in, w_out.T
    )
    own = part_in.shape[0] // devices
    sends = jnp.concatenate(
        [part_in.reshape(devices, own, width), part_out.reshape(devices, own, width)], axis=1
    )
    got = exchange(sends, AXES, 2)
    total = jnp.sum(got.astype(F32), axis=0)
    return jnp.swapaxes(output, 1, 2)[None], total[:own].T, total[own:]


def solution(mesh):
    return jax.shard_map(
        per_device,
        mesh=mesh,
        in_specs=(
            P("tables", "cells", None, None),
            P("tables"),
            P("tables"),
            P(),
            P(),
            P(),
            P(),
            P(),
            P(),
            P("tables", "cells", None, None),
        ),
        out_specs=(
            P("tables", "cells", None, None),
            P(None, ("tables", "cells")),
            P(("tables", "cells"), None),
        ),
        check_vma=False,
    )
```
